32 devices in a mesh: row: 4 (over y, core), col: 4 (over z), dp: 2 (over x).
Axes of the slice: x: 2, y: 2, z: 4, core: 2. Of those that a mesh axis runs over, the one named last changes fastest.
Arguments:
- observed: bfloat16 [1024, 2048], P(('row', 'dp'), 'col'), may hold values from -6 to 6
- next_observed: bfloat16 [1024, 2048], P(('row', 'dp'), 'col'), may hold values from -6 to 6
- actions: bfloat16 [1024, 128], P(('row', 'dp')), may hold values from -1 to 1
- next_mean: bfloat16 [1024, 128], P(('row', 'dp')), may hold values from -1.1953125 to 1.1953125
- policy_noise: float32 [1024, 128], P(('row', 'dp')), may hold values from -1.5 to 1.5
- rewards: bfloat16 [1024], P(('row', 'dp')), may hold values from -5 to 5
- discounts: bfloat16 [1024], P(('row', 'dp')), may hold values from 0.5 to 0.98828125
- actor_flags: int32 [1024], P(('row', 'dp')), may hold values 0 or 1
- critic_in: float32 [2, 2048, 2048], P(None, 'col', 'row'), may hold values from -0.125 to 0.125
- critic_act: float32 [2, 128, 2048], P(None, None, 'col'), may hold values from -0.5 to 0.5
- critic_head: float32 [2, 2048], P(None, 'row'), may hold values from -0.125 to 0.125
- target_in: float32 [2, 2048, 2048], P(None, 'col', 'row'), may hold values from -0.125 to 0.125
- target_act: float32 [2, 128, 2048], P(None, None, 'col'), may hold values from -0.5 to 0.5
- target_head: float32 [2, 2048], P(None, 'row'), may hold values from -0.125 to 0.125
Outputs:
- new_in: float32 [2, 2048, 2048], P(None, 'col', 'row')
- new_act: float32 [2, 128, 2048], P(None, None, 'col')
- new_head: float32 [2, 2048], P(None, 'row')
- new_target_in: float32 [2, 2048, 2048], P(None, 'col', 'row')
- new_target_act: float32 [2, 128, 2048], P(None, None, 'col')
- new_target_head: float32 [2, 2048], P(None, 'row')
- temporal_errors: float32 [2, 1024], P(None, ('row', 'dp'))
- action_slope: float32 [1024, 128], P(('row', 'dp'))
The draws below stay inside these ranges and needn't reach their ends.
All inputs are finite; a program needn't handle non-finite values. No bound on the sum of `actor_flags` on one device may be relied on, other than what follows from the above.
Results may differ from the reference program's by a relative error of at most 0.008.
Values may be sent and summed in bfloat16 or wider, within the bound.
A program may use at most 128 MiB of HBM per device.

```python
import jax
import jax.numpy as jnp
from jax import lax

D = 2048
ACT = 128
TOKENS = 1024


def place_ends(drawn, rng, smallest, high):
    shape = drawn.shape
    index_at = [jax.random.randint(jax.random.fold_in(rng, axis), (), 0, shape[axis]) for axis in range(len(shape))]
    drawn = drawn.at[tuple(index_at)].set(smallest)
    longest = shape.index(max(shape))
    index_at[longest] = (index_at[longest] + 1) % shape[longest]
    return drawn.at[tuple(index_at)].set(high)


def level_of(key, dims, split, low, high):
    def one(dim, parts):
        draws = jax.random.uniform(jax.random.fold_in(jax.random.fold_in(key, 6), dim), (parts,), jnp.float32, low / len(split), high / len(split))
        return jnp.repeat(jnp.exp(draws), dims[dim] // parts).reshape((-1,) + (1,) * (len(dims) - dim - 1))

    factor_of = one(*split[0])
    for cut in split[1:]:
        factor_of = factor_of * one(*cut)
    return factor_of


def gaussian(own_key, shape, width, reach, pieces=(), held_as=jnp.bfloat16):
    values = jax.random.normal(own_key, shape, jnp.float32) * width
    if len(pieces) > 0:
        values = level_of(own_key, shape, pieces, -0.22, 0.18) * values
    return jnp.clip(values, min=-reach, max=reach).astype(held_as)


def setup_inputs(seed: int = 0) -> dict:
    seeds = jax.random.split(jax.random.key(seed), 15)
    return {
        "observed": gaussian(seeds[0], (TOKENS, D), 1.0, 6.0, ((0, 8), (1, 4))),
        "next_observed": gaussian(seeds[1], (TOKENS, D), 1.0, 6.0, ((0, 8), (1, 4))),
        "actions": jnp.clip(jax.random.uniform(seeds[2], (TOKENS, ACT), jnp.float32, -1.0, 1.0) * level_of(seeds[2], (TOKENS, ACT), ((0, 8),), -0.4, 0.0), -1.0, 1.0).astype(jnp.bfloat16),
        "next_mean": jnp.clip(jax.random.uniform(seeds[3], (TOKENS, ACT), jnp.float32, -1.1953125, 1.1953125) * level_of(seeds[3], (TOKENS, ACT), ((0, 8),), -0.4, 0.0), -1.1953125, 1.1953125).astype(jnp.bfloat16),
        "policy_noise": gaussian(seeds[4], (TOKENS, ACT), 0.3, 1.5, ((0, 8),), jnp.float32),
        "rewards": gaussian(seeds[5], (TOKENS,), 1.0, 5.0, ((0, 8),)),
        "discounts": jnp.clip(0.5 + 0.48828125 * jax.random.uniform(seeds[6], (TOKENS,), jnp.float32) ** level_of(seeds[6], (TOKENS,), ((0, 8),), -0.2, 0.2), 0.5, 0.98828125).astype(jnp.bfloat16),
        "actor_flags": place_ends((jax.random.randint(seeds[7], (TOKENS,), 0, 2) < 1).astype(jnp.int32), jax.random.fold_in(seeds[7], 1), 0, 1),
        "critic_in": gaussian(seeds[8], (2, D, D), D ** -0.5, 0.125, ((1, 4), (2, 4)), jnp.float32),
        "critic_act": gaussian(seeds[9], (2, ACT, D), ACT ** -0.5, 0.5, ((2, 4),), jnp.float32),
        "critic_head": gaussian(seeds[10], (2, D), D ** -0.5, 0.125, ((1, 4),), jnp.float32),
        "target_in": gaussian(seeds[11], (2, D, D), D ** -0.5, 0.125, ((1, 4), (2, 4)), jnp.float32),
        "target_act": gaussian(seeds[12], (2, ACT, D), ACT ** -0.5, 0.5, ((2, 4),), jnp.float32),
        "target_head": gaussian(seeds[13], (2, D), D ** -0.5, 0.125, ((1, 4),), jnp.float32),
    }


noise_clip = 0.5
matrix_rate = 0.004
head_rate = 0.0001
blend_rate = 0.005


def silu_slope(preact):
    sigma = jax.nn.sigmoid(preact)
    return sigma * (1.0 + preact * (1.0 - sigma))


def forward(states, moves, weight_in, weight_act, weight_head):
    embedded = (states.astype(jnp.float32) + jnp.dot(moves, weight_act.astype(jnp.bfloat16), preferred_element_type=jnp.float32)).astype(jnp.bfloat16)
    preact = jnp.dot(embedded, weight_in.astype(jnp.bfloat16), preferred_element_type=jnp.float32)
    hidden = jax.nn.silu(preact)
    value = jnp.dot(hidden, weight_head, precision=lax.Precision.HIGHEST)
    return embedded, preact, hidden, value


def reference(observed, next_observed, actions, next_mean, policy_noise, rewards, discounts, actor_flags, critic_in, critic_act, critic_head, target_in, target_act, target_head):
    noisy = jnp.clip(next_mean.astype(jnp.float32) + jnp.clip(policy_noise, -noise_clip, noise_clip), -1.0, 1.0).astype(jnp.bfloat16)
    target_zero = forward(next_observed, noisy, target_in[0], target_act[0], target_head[0])[3]
    target_one = forward(next_observed, noisy, target_in[1], target_act[1], target_head[1])[3]
    goal = rewards.astype(jnp.float32) + discounts.astype(jnp.float32) * jnp.minimum(target_zero, target_one)
    fresh_in = []
    fresh_act = []
    fresh_head = []
    errors = []
    action_slope = None
    for which in range(2):
        embedded, preact, hidden, value = forward(observed, actions, critic_in[which], critic_act[which], critic_head[which])
        error = value - goal
        slope = (critic_head[which] * silu_slope(preact)).astype(jnp.bfloat16)
        delta = (2.0 * error[:, None] * slope.astype(jnp.float32)).astype(jnp.bfloat16)
        back = jnp.dot(slope, critic_in[which].astype(jnp.bfloat16).T, preferred_element_type=jnp.float32)
        grad_embedded = (2.0 * error[:, None] * back).astype(jnp.bfloat16)
        grad_in = jnp.dot(embedded.T, delta, preferred_element_type=jnp.float32)
        grad_act = jnp.dot(actions.T, grad_embedded, preferred_element_type=jnp.float32)
        grad_head = jnp.dot(2.0 * error, hidden, precision=lax.Precision.HIGHEST)
        fresh_in.append(critic_in[which] - matrix_rate * grad_in)
        fresh_act.append(critic_act[which] - matrix_rate * grad_act)
        fresh_head.append(critic_head[which] - head_rate * grad_head)
        errors.append(error)
        if which == 0:
            push = jnp.dot(back.astype(jnp.bfloat16), critic_act[0].astype(jnp.bfloat16).T, preferred_element_type=jnp.float32)
            action_slope = actor_flags.astype(jnp.float32)[:, None] * push
    new_in = jnp.stack(fresh_in)
    new_act = jnp.stack(fresh_act)
    new_head = jnp.stack(fresh_head)
    new_target_in = blend_rate * new_in + (1.0 - blend_rate) * target_in
    new_target_act = blend_rate * new_act + (1.0 - blend_rate) * target_act
    new_target_head = blend_rate * new_head + (1.0 - blend_rate) * target_head
    return new_in, new_act, new_head, new_target_in, new_target_act, new_target_head, jnp.stack(errors), action_slope
```

```python
import functools

import jax
import jax.numpy as jnp
from jax import lax
from jax.experimental import pallas as pl
from jax.experimental.pallas import tpu as pltpu
from jax.sharding import PartitionSpec as P

noise_clip = 0.5
matrix_rate = 0.004
head_rate = 0.0001
blend_rate = 0.005

f32 = jnp.float32
bf16 = jnp.bfloat16
skew = 3


def kernel(dims, on_own, tg_own, cin, tin, cact, tact, heads, g_in, g_act, g_head, errs_out, push_out,
           w16, a16, on_all, tg_all, emb, slopes, delta, rs_out, rs_in, hidden, vals, vt_own, vt_in,
           errs, gh, epad, ga_own, ga_out, ga_in, ga_all, pu_out, pu_in, pz_all,
           on_s, on_r, tg_s, tg_r, fon_s, fon_r, ftg_s, ftg_r, xon_s, xon_r,
           rs_s, rs_r, sl_s, sl_r, xs_s, xs_r, vt_s, vt_r, er_s, er_r, gh_s, gh_r,
           ga_s, ga_r, gb_s, gb_r, pu_s, pu_r, pz_s, pz_r):
    R, C, D, TB, F, H, A = dims
    HI = R // 2
    TC = TB // 2
    row, col, dp = lax.axis_index("row"), lax.axis_index("col"), lax.axis_index("dp")
    hi, lo = row // 2, row % 2
    n = 8 * HI
    m = n // 2

    def copy(src, dst, ssem, rsem, **where):
        return pltpu.make_async_remote_copy(
            src_ref=src, dst_ref=dst, send_sem=ssem, recv_sem=rsem,
            device_id=where, device_id_type=pl.DeviceIdType.MESH)

    plane = [(c, d) for d in range(D) for c in range(C) if c or d]
    barrier = pltpu.get_barrier_semaphore()
    for o in range(1, R):
        pl.semaphore_signal(barrier, inc=1, device_id={"row": (row + o) % R},
                            device_id_type=pl.DeviceIdType.MESH)
    for c, d in plane:
        pl.semaphore_signal(barrier, inc=1,
                            device_id={"col": (col + c) % C, "dp": (dp + d) % D},
                            device_id_type=pl.DeviceIdType.MESH)
    pl.semaphore_wait(barrier, R - 1 + len(plane))

    def on_copy(o):
        to = hi * 2 + (1 - lo) if o == 0 else ((hi + o) % HI) * 2 + lo
        return copy(on_own, on_all.at[dp, row], on_s.at[o], on_r.at[o], row=to)

    def tg_copy(o):
        to = hi * 2 + (1 - lo) if o == 0 else ((hi + o) % HI) * 2 + lo
        return copy(tg_own, tg_all.at[row], tg_s.at[o], tg_r.at[o], row=to)

    for o in range(HI):
        on_copy(o).start()
    for o in range(HI):
        tg_copy(o).start()
    on_all[dp, row] = on_own[...]
    tg_all[row] = tg_own[...]
    for k in range(2):
        w16[k] = cin[k].astype(bf16)
        w16[2 + k] = tin[k].astype(bf16)
        a16[k] = cact[k].astype(bf16)
        a16[2 + k] = tact[k].astype(bf16)

    def fon_copy(o, block):
        return copy(on_all.at[dp, block], on_all.at[dp, block], fon_s.at[o], fon_r.at[o],
                    row=hi * 2 + (1 - lo))

    def ftg_copy(o, block):
        return copy(tg_all.at[block], tg_all.at[block], ftg_s.at[o], ftg_r.at[o],
                    row=hi * 2 + (1 - lo))

    def xon_copy(a, o, block, e):
        return copy(on_all.at[dp, block], on_all.at[dp, block], xon_s.at[a, o, e - 1],
                    xon_r.at[a, o, e - 1], dp=(dp + e) % D)

    def rows_of(d, block):
        return pl.ds(pl.multiple_of((d * R + block) * TB, TB), TB)

    def embed_on(d, block):
        x = on_all[d, block]
        for k in range(2):
            mixed = jnp.dot(x[:, F:], a16[k], preferred_element_type=f32)
            emb[k, rows_of(d, block), :] = (x[:, :F].astype(f32) + mixed).astype(bf16)

    def embed_tg(block):
        x = tg_all[block]
        for k in range(2):
            mixed = jnp.dot(x[:, F:F + A], a16[2 + k], preferred_element_type=f32)
            emb[k, rows_of(D, block), :] = (x[:, :F].astype(f32) + mixed).astype(bf16)

    def prepare(a, i):
        block_of = lambda o: ((hi + o) % HI) * 2 + a
        for o in range(HI):
            block = block_of(o)

            @pl.when(i == 4 * o)
            def _():
                @pl.when(lo == a)
                def _():
                    if o > 0:
                        on_copy(o).wait_recv()
                        fon_copy(o, block).start()

                @pl.when(lo != a)
                def _():
                    if o > 0:
                        fon_copy(o, block).wait_recv()
                    else:
                        on_copy(0).wait_recv()
                for e in range(1, D):
                    xon_copy(a, o, block, e).start()
                embed_on(dp, block)

            @pl.when(i == 4 * (HI + o))
            def _():
                @pl.when(lo == a)
                def _():
                    if o > 0:
                        tg_copy(o).wait_recv()
                        ftg_copy(o, block).start()

                @pl.when(lo != a)
                def _():
                    if o > 0:
                        ftg_copy(o, block).wait_recv()
                    else:
                        tg_copy(0).wait_recv()
                embed_tg(block)

    def place(a, i):
        group = i // (4 * HI)
        o = (i // 4) % HI
        kk = (i // 2) % 2
        half = i % 2
        there = (hi + o) % HI
        return group, kk, half, there, there * 2 + a

    def rs_copy(a, i):
        to = (col + 1) % C if a == 0 else (col + C - 1) % C
        return copy(rs_out.at[a, i], rs_in.at[a, i], rs_s.at[a, i], rs_r.at[a, i], col=to)

    def slope_at(d, kk, block, half):
        start = (d * R + block) * TB + half * TC
        return slopes.at[kk, pl.ds(pl.multiple_of(start, TC), TC), :]

    def sl_copy(a, j):
        _, kk, half, there, block = place(a, j)
        at = slope_at(dp, kk, block, half)
        to = (col + C - 1) % C if a == 0 else (col + 1) % C
        return copy(at, at, sl_s.at[a, j], sl_r.at[a, j], col=to)

    def xs_copy(a, j, e):
        _, kk, half, there, block = place(a, j)
        at = slope_at(dp, kk, block, half)
        return copy(at, at, xs_s.at[a, j, e - 1], xs_r.at[a, j, e - 1], dp=(dp + e) % D)

    lane = lax.broadcasted_iota(jnp.int32, (TC, 128), 1)

    def finish(a, i, pre):
        group, kk, half, there, block = place(a, i)
        sigma = jax.nn.sigmoid(pre)
        hid = pre * sigma
        head = heads[group * 2 + kk]
        value = jnp.sum(hid * head, axis=1, keepdims=True)
        at = pl.ds(pl.multiple_of(there * TB + half * TC, TC), TC)
        vals[at, :] += jnp.where(lane == group * 2 + kk, value, 0.0)

        @pl.when(group == 0)
        def _():
            hidden[kk, at, :] = hid.astype(bf16)
            start = (dp * R + block) * TB + half * TC
            slopes[kk, pl.ds(pl.multiple_of(start, TC), TC), :] = (
                head * (sigma * (1.0 + pre * (1.0 - sigma)))).astype(bf16)
            sl_copy(a, i).start()
            for e in range(1, D):
                xs_copy(a, i, e).start()

    vals[...] = jnp.zeros_like(vals)

    def step(s, carry):
        for a in range(2):
            far = col if a == 0 else C - 1 - col
            i = s - skew * far

            @pl.when((i >= 0) & (i < n))
            def _():
                prepare(a, i)
                group, kk, half, there, block = place(a, i)
                start = (jnp.where(group == 0, dp, D) * R + block) * TB + half * TC

                def partial():
                    left = emb[kk, pl.ds(pl.multiple_of(start, TC), TC), :]
                    return jnp.dot(left, w16[group * 2 + kk], preferred_element_type=f32)

                @pl.when(far == 0)
                def _():
                    rs_out[a, i] = partial().astype(bf16)
                    rs_copy(a, i).start()

                @pl.when((far > 0) & (far < C - 1))
                def _():
                    mine = partial()
                    rs_copy(a, i).wait_recv()
                    rs_out[a, i] = (mine + rs_in[a, i].astype(f32)).astype(bf16)
                    rs_copy(a, i).start()

                @pl.when(far == C - 1)
                def _():
                    mine = partial()
                    rs_copy(a, i).wait_recv()
                    finish(a, i, mine + rs_in[a, i].astype(f32))

            j = s - skew * (2 * (C - 1) - far)

            @pl.when((j >= 0) & (j < m) & (far < C - 1))
            def _():
                sl_copy(a, j).wait_recv()

                @pl.when(far > 0)
                def _():
                    sl_copy(a, j).start()
                for e in range(1, D):
                    xs_copy(a, j, e).start()
        return carry

    lax.fori_loop(0, n + skew * (C - 1), step, 0)

    def vt_copy(o):
        return copy(vt_own, vt_in.at[o - 1], vt_s.at[o - 1], vt_r.at[o - 1], row=(row + o) % R)

    def er_copy(x, a):
        c, d = plane[x]
        return copy(errs.at[dp, a], errs.at[dp, a], er_s.at[x], er_r.at[a, x],
                    col=(col + c) % C, dp=(dp + d) % D)

    def gh_copy(x, a):
        c, d = plane[x]
        return copy(gh.at[dp, a], gh.at[dp, a], gh_s.at[x], gh_r.at[a, x],
                    col=(col + c) % C, dp=(dp + d) % D)

    top = lax.broadcasted_iota(jnp.int32, (8, TB), 0)
    for a in range(2):
        @pl.when(col == (C - 1 if a == 0 else 0))
        def _():
            own = []
            for h in range(HI):
                seen = vals[h * TB:(h + 1) * TB, :] + tg_all[h * 2 + a][:, F + A:].astype(f32)
                own.append(seen.T[:8])
                vt_own[h] = own[h]
            for o in range(1, R):
                vt_copy(o).start()
            for o in range(1, R):
                vt_copy(o).wait()
            total = jnp.zeros((8, H), f32)
            for h in range(HI):
                summed = own[h]
                for o in range(1, R):
                    summed = summed + vt_in[o - 1, h]
                goal = own[h][4:5] + own[h][5:6] * jnp.minimum(summed[2:3], summed[3:4])
                err = jnp.where(top < 2, summed - goal, 0.0)
                errs[dp, a, h] = err
                twice = (2.0 * err).astype(bf16)
                for k in range(2):
                    got = jnp.dot(twice, hidden[k, h * TB:(h + 1) * TB, :],
                                  preferred_element_type=f32)
                    keep = lax.broadcasted_iota(jnp.int32, (8, H), 0) == k
                    total = total + jnp.where(keep, got, 0.0)
            for x in range(len(plane)):
                er_copy(x, a).start()
            gh[dp, a] = total
            for x in range(len(plane)):
                gh_copy(x, a).start()

    def late(s, carry):
        for a in range(2):
            far = col if a == 0 else C - 1 - col
            j = s - skew * (2 * (C - 1) - far)

            @pl.when((j >= 0) & (j < m) & (far < C - 1))
            def _():
                sl_copy(a, j).wait_recv()

                @pl.when(far > 0)
                def _():
                    sl_copy(a, j).start()
                for e in range(1, D):
                    xs_copy(a, j, e).start()
        return carry

    lax.fori_loop(n + skew * (C - 1), max(n + skew * (C - 1), m + 2 * skew * (C - 1)), late, 0)

    def pu_copy(o):
        return copy(pu_out.at[o], pu_in.at[o - 1], pu_s.at[o - 1], pu_r.at[o - 1],
                    row=(row + o) % R)

    def pz_copy(c):
        return copy(pz_all.at[col], pz_all.at[col], pz_s.at[c - 1], pz_r.at[c - 1],
                    col=(col + c) % C)

    lift = jnp.dot(a16[0], w16[0], preferred_element_type=f32).astype(bf16)
    last = (((1,), (1,)), ((), ()))
    first = (((0,), (0,)), ((), ()))
    own_push = None
    for o in range(R):
        got = lax.dot_general(slopes[0, rows_of(dp, (row + o) % R), :], lift, last,
                              preferred_element_type=f32)
        if o == 0:
            own_push = got
        else:
            pu_out[o] = got.astype(bf16)
            pu_copy(o).start()

    for e in range(1, D):
        src = (dp + D - e) % D
        for a in range(2):
            for o in range(HI):
                block = ((hi + o) % HI) * 2 + a
                xon_copy(a, o, block, e).wait_recv()
                embed_on(src, block)

    for o in range(1, R):
        pu_copy(o).wait_recv()
        own_push = own_push + pu_in[o - 1].astype(f32)
    pz_all[col] = own_push.astype(bf16)
    for c in range(1, C):
        pz_copy(c).start()

    for e in range(1, D):
        def take(j, carry):
            for a in range(2):
                xs_copy(a, j, e).wait_recv()
            return carry
        lax.fori_loop(0, m, take, 0)

    for a in range(2):
        end = C - 1 if a == 0 else 0
        for x, (c, d) in enumerate(plane):
            @pl.when((col + C - c) % C == end)
            def _():
                er_copy(x, a).wait_recv()

    epad[...] = jnp.zeros_like(epad)
    for d in range(D):
        for h in range(HI):
            for a in range(2):
                epad[0:8, :] = 2.0 * errs[d, a, h]
                column = epad[...].T
                at = slice((d * R + h * 2 + a) * TB, (d * R + h * 2 + a + 1) * TB)
                for k in range(2):
                    scaled = column[:, k:k + 1] * slopes[k, at, :].astype(f32)
                    delta[k, at, :] = scaled.astype(bf16)

    FR = F // R

    def ga_copy(o):
        to = (row + o) % R
        return copy(ga_out.at[to], ga_in.at[o - 1], ga_s.at[o - 1], ga_r.at[o - 1], row=to)

    def gb_copy(o):
        return copy(ga_all.at[row], ga_all.at[row], gb_s.at[o - 1], gb_r.at[o - 1],
                    row=(row + o) % R)

    for k in range(2):
        moved = jnp.zeros((A, H), f32)
        for d in range(D):
            for b in range(R):
                at = slice((d * R + b) * TB, (d * R + b + 1) * TB)
                moved = moved + lax.dot_general(on_all[d, b][:, F:], delta[k, at, :], first,
                                                preferred_element_type=f32)
        term = lax.dot_general(moved.astype(bf16), w16[k], last, preferred_element_type=f32)
        for p in range(R):
            piece = term[:, p * FR:(p + 1) * FR]
            ga_own[p, k] = piece
            ga_out[p, k] = piece.astype(bf16)
    for o in range(1, R):
        ga_copy(o).start()

    def grad_in(k):
        g_in[k] = jnp.zeros((F, H), f32)

        def add(d, carry):
            at = pl.ds(pl.multiple_of(d * R * TB, R * TB), R * TB)
            g_in[k] += lax.dot_general(emb[k, at, :], delta[k, at, :], first,
                                       preferred_element_type=f32)
            return carry
        lax.fori_loop(0, D, add, 0)

    grad_in(0)
    for o in range(1, R):
        ga_copy(o).wait_recv()
    for k in range(2):
        piece = ga_own[row, k]
        for o in range(1, R):
            piece = piece + ga_in[o - 1, k].astype(f32)
        ga_all[row, k] = piece.astype(bf16)
    for o in range(1, R):
        gb_copy(o).start()
    grad_in(1)

    for c in range(1, C):
        pz_copy(c).wait_recv()
    push = pz_all[0].astype(f32)
    for c in range(1, C):
        push = push + pz_all[c].astype(f32)
    push_out[...] = push
    errs_out[...] = errs[dp, lo, hi]

    for a in range(2):
        end = C - 1 if a == 0 else 0
        for x, (c, d) in enumerate(plane):
            @pl.when((col + C - c) % C == end)
            def _():
                gh_copy(x, a).wait_recv()
    whole = gh[0, 0]
    for d in range(D):
        for a in range(2):
            if d or a:
                whole = whole + gh[d, a]
    g_head[...] = whole

    for o in range(1, R):
        gb_copy(o).wait_recv()
    for p in range(R):
        for k in range(2):
            g_act[k, :, p * FR:(p + 1) * FR] = ga_all[p, k].astype(f32)

    for o in range(HI):
        on_copy(o).wait_send()
        tg_copy(o).wait_send()
        if o > 0:
            fon_copy(o, row).wait_send()
            ftg_copy(o, row).wait_send()
        for a in range(2):
            for e in range(1, D):
                xon_copy(a, o, row, e).wait_send()
    for a in range(2):
        far = col if a == 0 else C - 1 - col

        @pl.when(far < C - 1)
        def _():
            def left(i, carry):
                rs_copy(a, i).wait_send()
                return carry
            lax.fori_loop(0, n, left, 0)

        @pl.when(far > 0)
        def _():
            def left(j, carry):
                sl_copy(a, j).wait_send()
                return carry
            lax.fori_loop(0, m, left, 0)

        def gone(j, carry):
            for e in range(1, D):
                xs_copy(a, j, e).wait_send()
            return carry
        lax.fori_loop(0, m, gone, 0)

        @pl.when(far == C - 1)
        def _():
            for x in range(len(plane)):
                er_copy(x, a).wait_send()
                gh_copy(x, a).wait_send()
    for o in range(1, R):
        pu_copy(o).wait_send()
        ga_copy(o).wait_send()
        gb_copy(o).wait_send()
    for c in range(1, C):
        pz_copy(c).wait_send()


def on_device(dims, observed, next_observed, actions, next_mean, policy_noise, rewards, discounts,
              actor_flags, critic_in, critic_act, critic_head, target_in, target_act, target_head):
    R, C, D, TB, F, H, A = dims
    HI, TC = R // 2, TB // 2
    n, m, planes = 8 * HI, 4 * HI, C * D - 1
    noisy = jnp.clip(
        next_mean.astype(f32) + jnp.clip(policy_noise, -noise_clip, noise_clip), -1.0, 1.0
    ).astype(bf16)
    lanes = lax.broadcasted_iota(jnp.int32, (TB, 128), 1)
    zero = jnp.zeros((), bf16)
    extra = jnp.where(lanes == 4, rewards[:, None],
                      jnp.where(lanes == 5, discounts[:, None], zero))
    on_own = jnp.concatenate([observed, actions], axis=1)
    tg_own = jnp.concatenate([next_observed, noisy, extra], axis=1)
    heads = jnp.concatenate([critic_head, target_head], axis=0)[:, None, :]
    dma = lambda *shape: pltpu.SemaphoreType.DMA(shape)
    vmem = pltpu.VMEM
    scratch = [
        vmem((4, F, H), bf16), vmem((4, A, F), bf16),
        vmem((D, R, TB, F + A), bf16), vmem((R, TB, F + A + 128), bf16),
        vmem((2, (D + 1) * R * TB, F), bf16),
        vmem((2, D * R * TB, H), bf16), vmem((2, D * R * TB, H), bf16),
        vmem((2, n, TC, H), bf16), vmem((2, n, TC, H), bf16),
        vmem((2, HI * TB, H), bf16), vmem((HI * TB, 128), f32),
        vmem((HI, 8, TB), f32), vmem((R - 1, HI, 8, TB), f32),
        vmem((D, 2, HI, 8, TB), f32), vmem((D, 2, 8, H), f32), vmem((128, TB), f32),
        vmem((R, 2, A, F // R), f32), vmem((R, 2, A, F // R), bf16),
        vmem((R - 1, 2, A, F // R), bf16), vmem((R, 2, A, F // R), bf16),
        vmem((R, TB, A), bf16), vmem((R - 1, TB, A), bf16), vmem((C, TB, A), bf16),
        dma(HI), dma(HI), dma(HI), dma(HI),
        dma(HI), dma(HI), dma(HI), dma(HI),
        dma(2, HI, D - 1), dma(2, HI, D - 1),
        dma(2, n), dma(2, n), dma(2, m), dma(2, m),
        dma(2, m, D - 1), dma(2, m, D - 1),
        dma(R - 1), dma(R - 1),
        dma(planes), dma(2, planes), dma(planes), dma(2, planes),
        dma(R - 1), dma(R - 1), dma(R - 1), dma(R - 1),
        dma(R - 1), dma(R - 1), dma(C - 1), dma(C - 1),
    ]
    spec = pl.BlockSpec(memory_space=vmem)
    shaped = jax.ShapeDtypeStruct
    g_in, g_act, g_head, errors, push = pl.pallas_call(
        functools.partial(kernel, dims),
        out_shape=(shaped((2, F, H), f32), shaped((2, A, F), f32), shaped((8, H), f32),
                   shaped((8, TB), f32), shaped((TB, A), f32)),
        in_specs=[spec] * 7,
        out_specs=(spec,) * 5,
        scratch_shapes=scratch,
        compiler_params=pltpu.CompilerParams(
            collective_id=0, has_side_effects=True, vmem_limit_bytes=67043328),
    )(on_own, tg_own, critic_in, target_in, critic_act, target_act, heads)
    action_slope = push * actor_flags.astype(f32)[:, None]
    new_in = critic_in - matrix_rate * g_in
    new_act = critic_act - matrix_rate * g_act
    new_head = critic_head - head_rate * g_head[:2]
    new_target_in = blend_rate * new_in + (1.0 - blend_rate) * target_in
    new_target_act = blend_rate * new_act + (1.0 - blend_rate) * target_act
    new_target_head = blend_rate * new_head + (1.0 - blend_rate) * target_head
    return (new_in, new_act, new_head, new_target_in, new_target_act, new_target_head,
            errors[:2], action_slope)


def solution(mesh):
    def run(*args):
        R, C, D = mesh.shape["row"], mesh.shape["col"], mesh.shape["dp"]
        tokens, features = args[0].shape
        dims = (R, C, D, tokens // (R * D), features // C, args[8].shape[2] // R,
                args[2].shape[1])
        return sharded(dims)(*args)

    def sharded(dims):
        return jax.shard_map(
            functools.partial(on_device, dims),
            mesh=mesh,
            in_specs=(
                P(("row", "dp"), "col"),
                P(("row", "dp"), "col"),
                P(("row", "dp"), None),
                P(("row", "dp"), None),
                P(("row", "dp"), None),
                P(("row", "dp")),
                P(("row", "dp")),
                P(("row", "dp")),
                P(None, "col", "row"),
                P(None, None, "col"),
                P(None, "row"),
                P(None, "col", "row"),
                P(None, None, "col"),
                P(None, "row"),
            ),
            out_specs=(
                P(None, "col", "row"),
                P(None, None, "col"),
                P(None, "row"),
                P(None, "col", "row"),
                P(None, None, "col"),
                P(None, "row"),
                P(None, ("row", "dp")),
                P(("row", "dp"), None),
            ),
            check_vma=False,
        )

    return run
```

```python
import functools

import jax
import jax.numpy as jnp
from jax import lax
from jax.experimental import pallas as pl
from jax.experimental.pallas import tpu as pltpu
from jax.sharding import PartitionSpec as P

noise_clip = 0.5
matrix_rate = 0.004
head_rate = 0.0001
blend_rate = 0.005

f32 = jnp.float32
bf16 = jnp.bfloat16
skew = 2


def kernel(dims, observed, next_observed, actions, next_mean, noise, rewards, discounts, flags,
           cin, cact, chead, tin, tact, thead, new_in, new_act, new_head, new_tin, new_tact,
           new_thead, errs_out, push_out, on_own, tg_own, heads, flag_column, columns,
           w16, a16, on_all, tg_all, emb, slopes, delta, rs_out, rs_in, hidden, vals, vt_own, vt_in,
           errs, gh, epad, ga_own, ga_out, ga_in, ga_all, pu_out, pu_in, pz_all,
           on_s, on_r, tg_s, tg_r, fon_s, fon_r, ftg_s, ftg_r, xon_s, xon_r,
           rs_s, rs_r, sl_s, sl_r, xs_s, xs_r, vt_s, vt_r, er_s, er_r, gh_s, gh_r,
           ga_s, ga_r, gb_s, gb_r, pu_s, pu_r, pz_s, pz_r):
    R, C, D, TB, F, H, A = dims
    HI = R // 2
    TC = TB // 2
    row, col, dp = lax.axis_index("row"), lax.axis_index("col"), lax.axis_index("dp")
    hi, lo = row // 2, row % 2
    n = 8 * HI
    m = n // 2

    def copy(src, dst, ssem, rsem, **where):
        return pltpu.make_async_remote_copy(
            src_ref=src, dst_ref=dst, send_sem=ssem, recv_sem=rsem,
            device_id=where, device_id_type=pl.DeviceIdType.MESH)

    on_own[:, :F] = observed[...]
    on_own[:, F:] = actions[...]
    tg_own[:, :F] = next_observed[...]
    tg_own[:, F:F + A] = jnp.clip(
        next_mean[...].astype(f32) + jnp.clip(noise[...], -noise_clip, noise_clip), -1.0, 1.0
    ).astype(bf16)
    epad[...] = jnp.zeros_like(epad)
    epad[4:5, :] = rewards[...].astype(f32)
    epad[5:6, :] = discounts[...].astype(f32)
    tg_own[:, F + A:] = epad[...].T.astype(bf16)
    epad[0:1, :] = flags[...].astype(f32)
    flag_column[...] = epad[...].T[:, 0:1]
    for k in range(2):
        heads[k] = chead[k:k + 1, :]
        heads[2 + k] = thead[k:k + 1, :]

    plane = [(c, d) for d in range(D) for c in range(C) if c or d]
    barrier = pltpu.get_barrier_semaphore()
    for o in range(1, R):
        pl.semaphore_signal(barrier, inc=1, device_id={"row": (row + o) % R},
                            device_id_type=pl.DeviceIdType.MESH)
    for c, d in plane:
        pl.semaphore_signal(barrier, inc=1,
                            device_id={"col": (col + c) % C, "dp": (dp + d) % D},
                            device_id_type=pl.DeviceIdType.MESH)
    pl.semaphore_wait(barrier, R - 1 + len(plane))

    def on_copy(o):
        to = hi * 2 + (1 - lo) if o == 0 else ((hi + o) % HI) * 2 + lo
        return copy(on_own, on_all.at[dp, row], on_s.at[o], on_r.at[o], row=to)

    def tg_copy(o):
        to = hi * 2 + (1 - lo) if o == 0 else ((hi + o) % HI) * 2 + lo
        return copy(tg_own, tg_all.at[row], tg_s.at[o], tg_r.at[o], row=to)

    for o in range(HI):
        on_copy(o).start()
    for o in range(HI):
        tg_copy(o).start()
    on_all[dp, row] = on_own[...]
    tg_all[row] = tg_own[...]
    for k in range(2):
        w16[k] = cin[k].astype(bf16)
        w16[2 + k] = tin[k].astype(bf16)
        a16[k] = cact[k].astype(bf16)
        a16[2 + k] = tact[k].astype(bf16)

    def fon_copy(o, block):
        return copy(on_all.at[dp, block], on_all.at[dp, block], fon_s.at[o], fon_r.at[o],
                    row=hi * 2 + (1 - lo))

    def ftg_copy(o, block):
        return copy(tg_all.at[block], tg_all.at[block], ftg_s.at[o], ftg_r.at[o],
                    row=hi * 2 + (1 - lo))

    def xon_copy(a, o, block, e):
        return copy(on_all.at[dp, block], on_all.at[dp, block], xon_s.at[a, o, e - 1],
                    xon_r.at[a, o, e - 1], dp=(dp + e) % D)

    def rows_of(d, block):
        return pl.ds(pl.multiple_of((d * R + block) * TB, TB), TB)

    def embed_on(d, block):
        x = on_all[d, block]
        for k in range(2):
            mixed = jnp.dot(x[:, F:], a16[k], preferred_element_type=f32)
            emb[k, rows_of(d, block), :] = (x[:, :F].astype(f32) + mixed).astype(bf16)

    def embed_tg(block):
        x = tg_all[block]
        for k in range(2):
            mixed = jnp.dot(x[:, F:F + A], a16[2 + k], preferred_element_type=f32)
            emb[k, rows_of(D, block), :] = (x[:, :F].astype(f32) + mixed).astype(bf16)

    def prepare(a, i):
        block_of = lambda o: ((hi + o) % HI) * 2 + a
        for o in range(HI):
            block = block_of(o)

            @pl.when(i == 4 * o)
            def _():
                @pl.when(lo == a)
                def _():
                    if o > 0:
                        on_copy(o).wait_recv()
                        fon_copy(o, block).start()

                @pl.when(lo != a)
                def _():
                    if o > 0:
                        fon_copy(o, block).wait_recv()
                    else:
                        on_copy(0).wait_recv()
                for e in range(1, D):
                    xon_copy(a, o, block, e).start()
                embed_on(dp, block)

            @pl.when(i == 4 * (HI + o))
            def _():
                @pl.when(lo == a)
                def _():
                    if o > 0:
                        tg_copy(o).wait_recv()
                        ftg_copy(o, block).start()

                @pl.when(lo != a)
                def _():
                    if o > 0:
                        ftg_copy(o, block).wait_recv()
                    else:
                        tg_copy(0).wait_recv()
                embed_tg(block)

    def place(a, i):
        group = i // (4 * HI)
        o = (i // 4) % HI
        kk = (i // 2) % 2
        half = i % 2
        there = (hi + o) % HI
        return group, kk, half, there, there * 2 + a

    def rs_copy(a, i):
        to = (col + 1) % C if a == 0 else (col + C - 1) % C
        return copy(rs_out.at[a, i], rs_in.at[a, i], rs_s.at[a, i], rs_r.at[a, i], col=to)

    def slope_at(d, kk, block, half):
        start = (d * R + block) * TB + half * TC
        return slopes.at[kk, pl.ds(pl.multiple_of(start, TC), TC), :]

    def sl_copy(a, j):
        _, kk, half, there, block = place(a, j)
        at = slope_at(dp, kk, block, half)
        to = (col + C - 1) % C if a == 0 else (col + 1) % C
        return copy(at, at, sl_s.at[a, j], sl_r.at[a, j], col=to)

    def xs_copy(a, j, e):
        _, kk, half, there, block = place(a, j)
        at = slope_at(dp, kk, block, half)
        return copy(at, at, xs_s.at[a, j, e - 1], xs_r.at[a, j, e - 1], dp=(dp + e) % D)

    lane = lax.broadcasted_iota(jnp.int32, (TC, 128), 1)

    def finish(a, i, pre):
        group, kk, half, there, block = place(a, i)
        sigma = jax.nn.sigmoid(pre)
        hid = pre * sigma
        head = heads[group * 2 + kk]
        value = jnp.sum(hid * head, axis=1, keepdims=True)
        at = pl.ds(pl.multiple_of(there * TB + half * TC, TC), TC)
        vals[at, :] += jnp.where(lane == group * 2 + kk, value, 0.0)

        @pl.when(group == 0)
        def _():
            hidden[kk, at, :] = hid.astype(bf16)
            start = (dp * R + block) * TB + half * TC
            slopes[kk, pl.ds(pl.multiple_of(start, TC), TC), :] = (
                head * (sigma * (1.0 + pre * (1.0 - sigma)))).astype(bf16)
            sl_copy(a, i).start()
            for e in range(1, D):
                xs_copy(a, i, e).start()

    vals[...] = jnp.zeros_like(vals)

    def step(s, carry):
        for a in range(2):
            far = col if a == 0 else C - 1 - col
            i = s - skew * far

            @pl.when((i >= 0) & (i < n))
            def _():
                prepare(a, i)
                group, kk, half, there, block = place(a, i)
                start = (jnp.where(group == 0, dp, D) * R + block) * TB + half * TC

                def partial():
                    left = emb[kk, pl.ds(pl.multiple_of(start, TC), TC), :]
                    return jnp.dot(left, w16[group * 2 + kk], preferred_element_type=f32)

                @pl.when(far == 0)
                def _():
                    rs_out[a, i] = partial().astype(bf16)
                    rs_copy(a, i).start()

                @pl.when((far > 0) & (far < C - 1))
                def _():
                    mine = partial()
                    rs_copy(a, i).wait_recv()
                    rs_out[a, i] = (mine + rs_in[a, i].astype(f32)).astype(bf16)
                    rs_copy(a, i).start()

                @pl.when(far == C - 1)
                def _():
                    mine = partial()
                    rs_copy(a, i).wait_recv()
                    finish(a, i, mine + rs_in[a, i].astype(f32))

            j = s - skew * (2 * (C - 1) - far)

            @pl.when((j >= 0) & (j < m) & (far < C - 1))
            def _():
                sl_copy(a, j).wait_recv()

                @pl.when(far > 0)
                def _():
                    sl_copy(a, j).start()
                for e in range(1, D):
                    xs_copy(a, j, e).start()
        return carry

    lax.fori_loop(0, n + skew * (C - 1), step, 0)

    def vt_copy(o):
        return copy(vt_own, vt_in.at[o - 1], vt_s.at[o - 1], vt_r.at[o - 1], row=(row + o) % R)

    def er_copy(x, a):
        c, d = plane[x]
        return copy(errs.at[dp, a], errs.at[dp, a], er_s.at[x], er_r.at[a, x],
                    col=(col + c) % C, dp=(dp + d) % D)

    def gh_copy(x, a):
        c, d = plane[x]
        return copy(gh.at[dp, a], gh.at[dp, a], gh_s.at[x], gh_r.at[a, x],
                    col=(col + c) % C, dp=(dp + d) % D)

    top = lax.broadcasted_iota(jnp.int32, (8, TB), 0)
    for a in range(2):
        @pl.when(col == (C - 1 if a == 0 else 0))
        def _():
            own = []
            for h in range(HI):
                seen = vals[h * TB:(h + 1) * TB, :] + tg_all[h * 2 + a][:, F + A:].astype(f32)
                own.append(seen.T[:8])
                vt_own[h] = own[h]
            for o in range(1, R):
                vt_copy(o).start()
            for o in range(1, R):
                vt_copy(o).wait()
            total = jnp.zeros((8, H), f32)
            for h in range(HI):
                summed = own[h]
                for o in range(1, R):
                    summed = summed + vt_in[o - 1, h]
                goal = own[h][4:5] + own[h][5:6] * jnp.minimum(summed[2:3], summed[3:4])
                err = jnp.where(top < 2, summed - goal, 0.0)
                errs[dp, a, h] = err
                twice = (2.0 * err).astype(bf16)
                for k in range(2):
                    got = jnp.dot(twice, hidden[k, h * TB:(h + 1) * TB, :],
                                  preferred_element_type=f32)
                    keep = lax.broadcasted_iota(jnp.int32, (8, H), 0) == k
                    total = total + jnp.where(keep, got, 0.0)
            for x in range(len(plane)):
                er_copy(x, a).start()
            gh[dp, a] = total
            for x in range(len(plane)):
                gh_copy(x, a).start()

    def late(s, carry):
        for a in range(2):
            far = col if a == 0 else C - 1 - col
            j = s - skew * (2 * (C - 1) - far)

            @pl.when((j >= 0) & (j < m) & (far < C - 1))
            def _():
                sl_copy(a, j).wait_recv()

                @pl.when(far > 0)
                def _():
                    sl_copy(a, j).start()
                for e in range(1, D):
                    xs_copy(a, j, e).start()
        return carry

    lax.fori_loop(n + skew * (C - 1), max(n + skew * (C - 1), m + 2 * skew * (C - 1)), late, 0)

    def pu_copy(o):
        return copy(pu_out.at[o], pu_in.at[o - 1], pu_s.at[o - 1], pu_r.at[o - 1],
                    row=(row + o) % R)

    def pz_copy(c):
        return copy(pz_all.at[col], pz_all.at[col], pz_s.at[c - 1], pz_r.at[c - 1],
                    col=(col + c) % C)

    lift = jnp.dot(a16[0], w16[0], preferred_element_type=f32).astype(bf16)
    last = (((1,), (1,)), ((), ()))
    first = (((0,), (0,)), ((), ()))
    own_push = None
    for o in range(R):
        got = lax.dot_general(slopes[0, rows_of(dp, (row + o) % R), :], lift, last,
                              preferred_element_type=f32)
        if o == 0:
            own_push = got
        else:
            pu_out[o] = got.astype(bf16)
            pu_copy(o).start()

    for e in range(1, D):
        src = (dp + D - e) % D
        for a in range(2):
            for o in range(HI):
                block = ((hi + o) % HI) * 2 + a
                xon_copy(a, o, block, e).wait_recv()
                embed_on(src, block)

    for o in range(1, R):
        pu_copy(o).wait_recv()
        own_push = own_push + pu_in[o - 1].astype(f32)
    pz_all[col] = own_push.astype(bf16)
    for c in range(1, C):
        pz_copy(c).start()

    for e in range(1, D):
        def take(j, carry):
            for a in range(2):
                xs_copy(a, j, e).wait_recv()
            return carry
        lax.fori_loop(0, m, take, 0)

    for a in range(2):
        end = C - 1 if a == 0 else 0
        for x, (c, d) in enumerate(plane):
            @pl.when((col + C - c) % C == end)
            def _():
                er_copy(x, a).wait_recv()

    epad[...] = jnp.zeros_like(epad)
    for d in range(D):
        for h in range(HI):
            for a in range(2):
                epad[0:8, :] = 2.0 * errs[d, a, h]
                at = slice((d * R + h * 2 + a) * TB, (d * R + h * 2 + a + 1) * TB)
                columns[at, :] = epad[...].T

    FR = F // R

    def ga_copy(o):
        to = (row + o) % R
        return copy(ga_out.at[to], ga_in.at[o - 1], ga_s.at[o - 1], ga_r.at[o - 1], row=to)

    def gb_copy(o):
        return copy(ga_all.at[row], ga_all.at[row], gb_s.at[o - 1], gb_r.at[o - 1],
                    row=(row + o) % R)

    for k in range(2):
        moved = jnp.zeros((A, H), f32)
        for d in range(D):
            for b in range(R):
                at = slice((d * R + b) * TB, (d * R + b + 1) * TB)
                scaled = columns[at, k:k + 1] * on_all[d, b][:, F:].astype(f32)
                moved = moved + lax.dot_general(scaled.astype(bf16), slopes[k, at, :], first,
                                                preferred_element_type=f32)
        term = lax.dot_general(moved.astype(bf16), w16[k], last, preferred_element_type=f32)
        for p in range(R):
            piece = term[:, p * FR:(p + 1) * FR]
            ga_own[p, k] = piece
            ga_out[p, k] = piece.astype(bf16)
    for o in range(1, R):
        ga_copy(o).start()

    def blend(fresh, target):
        return blend_rate * fresh + (1.0 - blend_rate) * target

    def grad_in(k):
        for b in range(D * R):
            at = slice(b * TB, (b + 1) * TB)
            scaled = columns[at, k:k + 1] * slopes[k, at, :].astype(f32)
            delta[k, at, :] = scaled.astype(bf16)

        def add(d, carry):
            at = pl.ds(pl.multiple_of(d * R * TB, R * TB), R * TB)
            new_in[k] += lax.dot_general(emb[k, at, :], delta[k, at, :], first,
                                         preferred_element_type=f32)
            return carry
        new_in[k] = lax.dot_general(emb[k, :R * TB, :], delta[k, :R * TB, :], first,
                                    preferred_element_type=f32)
        lax.fori_loop(1, D, add, 0)
        fresh = cin[k] - matrix_rate * new_in[k]
        new_in[k] = fresh
        new_tin[k] = blend(fresh, tin[k])

    grad_in(0)
    for o in range(1, R):
        ga_copy(o).wait_recv()
    for k in range(2):
        piece = ga_own[row, k]
        for o in range(1, R):
            piece = piece + ga_in[o - 1, k].astype(f32)
        ga_all[row, k] = piece.astype(bf16)
    for o in range(1, R):
        gb_copy(o).start()
    grad_in(1)

    for c in range(1, C):
        pz_copy(c).wait_recv()
    push = pz_all[0].astype(f32)
    for c in range(1, C):
        push = push + pz_all[c].astype(f32)
    push_out[...] = push * flag_column[...]
    errs_out[...] = errs[dp, lo, hi, 0:2, :]

    for a in range(2):
        end = C - 1 if a == 0 else 0
        for x, (c, d) in enumerate(plane):
            @pl.when((col + C - c) % C == end)
            def _():
                gh_copy(x, a).wait_recv()
    whole = gh[0, 0]
    for d in range(D):
        for a in range(2):
            if d or a:
                whole = whole + gh[d, a]
    new_head[...] = chead[...] - head_rate * whole[:2]
    new_thead[...] = blend(new_head[...], thead[...])

    for o in range(1, R):
        gb_copy(o).wait_recv()
    for p in range(R):
        for k in range(2):
            part = slice(p * FR, (p + 1) * FR)
            fresh = cact[k, :, part] - matrix_rate * ga_all[p, k].astype(f32)
            new_act[k, :, part] = fresh
            new_tact[k, :, part] = blend(fresh, tact[k, :, part])

    for o in range(HI):
        on_copy(o).wait_send()
        tg_copy(o).wait_send()
        if o > 0:
            fon_copy(o, row).wait_send()
            ftg_copy(o, row).wait_send()
        for a in range(2):
            for e in range(1, D):
                xon_copy(a, o, row, e).wait_send()
    for a in range(2):
        far = col if a == 0 else C - 1 - col

        @pl.when(far < C - 1)
        def _():
            def left(i, carry):
                rs_copy(a, i).wait_send()
                return carry
            lax.fori_loop(0, n, left, 0)

        @pl.when(far > 0)
        def _():
            def left(j, carry):
                sl_copy(a, j).wait_send()
                return carry
            lax.fori_loop(0, m, left, 0)

        def gone(j, carry):
            for e in range(1, D):
                xs_copy(a, j, e).wait_send()
            return carry
        lax.fori_loop(0, m, gone, 0)

        @pl.when(far == C - 1)
        def _():
            for x in range(len(plane)):
                er_copy(x, a).wait_send()
                gh_copy(x, a).wait_send()
    for o in range(1, R):
        pu_copy(o).wait_send()
        ga_copy(o).wait_send()
        gb_copy(o).wait_send()
    for c in range(1, C):
        pz_copy(c).wait_send()


def on_device(dims, observed, next_observed, actions, next_mean, policy_noise, rewards, discounts,
              actor_flags, critic_in, critic_act, critic_head, target_in, target_act, target_head):
    R, C, D, TB, F, H, A = dims
    HI, TC = R // 2, TB // 2
    n, m, planes = 8 * HI, 4 * HI, C * D - 1
    dma = lambda *shape: pltpu.SemaphoreType.DMA(shape)
    vmem = pltpu.VMEM
    scratch = [
        vmem((TB, F + A), bf16), vmem((TB, F + A + 128), bf16), vmem((4, 1, H), f32),
        vmem((TB, 1), f32), vmem((D * R * TB, 128), f32),
        vmem((4, F, H), bf16), vmem((4, A, F), bf16),
        vmem((D, R, TB, F + A), bf16), vmem((R, TB, F + A + 128), bf16),
        vmem((2, (D + 1) * R * TB, F), bf16),
        vmem((2, D * R * TB, H), bf16), vmem((2, D * R * TB, H), bf16),
        vmem((2, n, TC, H), bf16), vmem((2, n, TC, H), bf16),
        vmem((2, HI * TB, H), bf16), vmem((HI * TB, 128), f32),
        vmem((HI, 8, TB), f32), vmem((R - 1, HI, 8, TB), f32),
        vmem((D, 2, HI, 8, TB), f32), vmem((D, 2, 8, H), f32), vmem((128, TB), f32),
        vmem((R, 2, A, F // R), f32), vmem((R, 2, A, F // R), bf16),
        vmem((R - 1, 2, A, F // R), bf16), vmem((R, 2, A, F // R), bf16),
        vmem((R, TB, A), bf16), vmem((R - 1, TB, A), bf16), vmem((C, TB, A), bf16),
        dma(HI), dma(HI), dma(HI), dma(HI),
        dma(HI), dma(HI), dma(HI), dma(HI),
        dma(2, HI, D - 1), dma(2, HI, D - 1),
        dma(2, n), dma(2, n), dma(2, m), dma(2, m),
        dma(2, m, D - 1), dma(2, m, D - 1),
        dma(R - 1), dma(R - 1),
        dma(planes), dma(2, planes), dma(planes), dma(2, planes),
        dma(R - 1), dma(R - 1), dma(R - 1), dma(R - 1),
        dma(R - 1), dma(R - 1), dma(C - 1), dma(C - 1),
    ]
    spec = pl.BlockSpec(memory_space=vmem)
    shaped = jax.ShapeDtypeStruct
    return pl.pallas_call(
        functools.partial(kernel, dims),
        out_shape=(shaped((2, F, H), f32), shaped((2, A, F), f32), shaped((2, H), f32),
                   shaped((2, F, H), f32), shaped((2, A, F), f32), shaped((2, H), f32),
                   shaped((2, TB), f32), shaped((TB, A), f32)),
        in_specs=[spec] * 14,
        out_specs=(spec,) * 8,
        scratch_shapes=scratch,
        compiler_params=pltpu.CompilerParams(
            collective_id=0, has_side_effects=True, vmem_limit_bytes=67043328),
    )(observed, next_observed, actions, next_mean, policy_noise, rewards[None, :],
      discounts[None, :], actor_flags[None, :], critic_in, critic_act, critic_head, target_in,
      target_act, target_head)


def solution(mesh):
    def run(*args):
        R, C, D = mesh.shape["row"], mesh.shape["col"], mesh.shape["dp"]
        tokens, features = args[0].shape
        dims = (R, C, D, tokens // (R * D), features // C, args[8].shape[2] // R,
                args[2].shape[1])
        return sharded(dims)(*args)

    def sharded(dims):
        return jax.shard_map(
            functools.partial(on_device, dims),
            mesh=mesh,
            in_specs=(
                P(("row", "dp"), "col"),
                P(("row", "dp"), "col"),
                P(("row", "dp"), None),
                P(("row", "dp"), None),
                P(("row", "dp"), None),
                P(("row", "dp")),
                P(("row", "dp")),
                P(("row", "dp")),
                P(None, "col", "row"),
                P(None, None, "col"),
                P(None, "row"),
                P(None, "col", "row"),
                P(None, None, "col"),
                P(None, "row"),
            ),
            out_specs=(
                P(None, "col", "row"),
                P(None, None, "col"),
                P(None, "row"),
                P(None, "col", "row"),
                P(None, None, "col"),
                P(None, "row"),
                P(None, ("row", "dp")),
                P(("row", "dp"), None),
            ),
            check_vma=False,
        )

    return run
```
